32 devices in a mesh: dp: 4 (over y, z), tp: 8 (over x, core).
Axes of the slice: x: 4, y: 2, z: 2, core: 2. Of those that a mesh axis runs over, the one named last changes fastest.
The devices are a block of a 4x4x8 slice.
Arguments:
- x_steps: bfloat16 [4, 2048, 512], P(None, 'dp'), parts along dimension 1
- conv_state: bfloat16 [2048, 1024, 3], P('dp', 'tp'), parts along dimension 0
- ssm_state: float32 [2048, 1024, 16], P('dp', 'tp'), parts along dimension 0
- expert_ids: int32 [4, 2048, 1], P(None, 'dp'), parts along dimension 1
- g_in: bfloat16 [512], replicated
- w_in: bfloat16 [512, 2, 1024], P(None, None, 'tp')
- conv_w: bfloat16 [1024, 4], P('tp')
- conv_b: bfloat16 [1024], P('tp')
- w_xp: bfloat16 [1024, 64], P('tp')
- g_dt: bfloat16 [32], replicated
- g_b: bfloat16 [16], replicated
- g_c: bfloat16 [16], replicated
- w_dt: bfloat16 [32, 1024], P(None, 'tp')
- b_dt: bfloat16 [1024], P('tp')
- a_log: float32 [1024, 16], P('tp')
- d_skip: float32 [1024], P('tp')
- w_out: bfloat16 [1024, 512], P('tp')
- g_ff: bfloat16 [512], replicated
- w_router: bfloat16 [512, 16], replicated
- w_gate: bfloat16 [16, 512, 2048], P(None, None, 'tp')
- w_up: bfloat16 [16, 512, 2048], P(None, None, 'tp')
- w_down: bfloat16 [16, 2048, 512], P(None, 'tp')
Outputs:
- output 1: bfloat16 [4, 2048, 512], P(None, 'dp'), parts along dimension 1
- output 2: bfloat16 [2048, 1024, 3], P('dp', 'tp'), parts along dimension 0
- output 3: float32 [2048, 1024, 16], P('dp', 'tp'), parts along dimension 0
There are 4 independent parts. The reference program is written for one: setup_inputs(seed, part) draws one part's arguments, and reference() takes and returns one part's arrays. A program takes and returns all parts, laid end to end along the dimension named above; an argument that names none is the same for every part.
All inputs are finite; a program needn't handle non-finite values.
Results may differ from the reference program's by a relative error of at most 0.015917.
Values are sent between devices in bfloat16 or wider.
A program may use at most 768 MiB of HBM per device.

```python
import jax
import jax.numpy as jnp
from jax import lax

D_MODEL = 512
INNER = 1024
STATE_DIM = 16
DT_RANK = 32
FFN_DIM = 2048
EXPERTS = 16
TOP_K = 1
BATCH_SIZE = 512
NUM_STEPS = 4
CONV_WIDTH = 4
EPSILON = 1e-6


def gauss_draw(rng_key, arr_shape, std_scale):
    return jax.random.normal(rng_key, arr_shape, jnp.float32) * std_scale


def range_draw(rng_key, arr_shape, lower_end, upper_end):
    return jax.random.uniform(rng_key, arr_shape, jnp.float32, lower_end, upper_end)


def draw_routes(rng_key):
    key_jitter, key_skew = jax.random.split(rng_key)
    route_jitter = jax.random.randint(key_jitter, (NUM_STEPS, BATCH_SIZE, EXPERTS), 0, 64)
    expert_skew = jax.random.randint(key_skew, (EXPERTS,), 0, 96)
    cover_mask = (jnp.arange(NUM_STEPS)[:, None, None] == 0) & (jnp.arange(BATCH_SIZE)[None, :, None] == jnp.arange(EXPERTS)[None, None, :])
    scores = route_jitter + expert_skew[None, None, :] + jnp.where(cover_mask, 1000, 0)
    scores = scores * EXPERTS + jnp.arange(EXPERTS)[None, None, :]
    return lax.top_k(scores, TOP_K)[1].astype(jnp.int32)


def setup_inputs(seed: int = 0, part: int = 0) -> dict:
    base_key = jax.random.key(seed)
    part_keys = jax.random.split(jax.random.fold_in(base_key, part), 4)
    shared_keys = jax.random.split(base_key, 18)
    return {
        "x_steps": gauss_draw(part_keys[0], (NUM_STEPS, BATCH_SIZE, D_MODEL), 1.0).astype(jnp.bfloat16),
        "conv_state": gauss_draw(part_keys[1], (BATCH_SIZE, INNER, CONV_WIDTH - 1), 1.0).astype(jnp.bfloat16),
        "ssm_state": gauss_draw(part_keys[2], (BATCH_SIZE, INNER, STATE_DIM), 0.2),
        "expert_ids": draw_routes(part_keys[3]),
        "g_in": range_draw(shared_keys[0], (D_MODEL,), 0.4, 1.6).astype(jnp.bfloat16),
        "w_in": gauss_draw(shared_keys[1], (D_MODEL, 2, INNER), D_MODEL ** -0.5).astype(jnp.bfloat16),
        "conv_w": gauss_draw(shared_keys[2], (INNER, CONV_WIDTH), 0.5).astype(jnp.bfloat16),
        "conv_b": gauss_draw(shared_keys[3], (INNER,), 0.5).astype(jnp.bfloat16),
        "w_xp": gauss_draw(shared_keys[4], (INNER, DT_RANK + 2 * STATE_DIM), INNER ** -0.5).astype(jnp.bfloat16),
        "g_dt": range_draw(shared_keys[5], (DT_RANK,), 0.4, 1.6).astype(jnp.bfloat16),
        "g_b": range_draw(shared_keys[6], (STATE_DIM,), 0.4, 1.6).astype(jnp.bfloat16),
        "g_c": range_draw(shared_keys[7], (STATE_DIM,), 0.4, 1.6).astype(jnp.bfloat16),
        "w_dt": gauss_draw(shared_keys[8], (DT_RANK, INNER), 0.8 * DT_RANK ** -0.5).astype(jnp.bfloat16),
        "b_dt": (gauss_draw(shared_keys[9], (INNER,), 0.3) - 2.25).astype(jnp.bfloat16),
        "a_log": range_draw(shared_keys[10], (INNER, STATE_DIM), -0.7, 0.7),
        "d_skip": range_draw(shared_keys[11], (INNER,), 0.5, 1.5),
        "w_out": gauss_draw(shared_keys[12], (INNER, D_MODEL), INNER ** -0.5).astype(jnp.bfloat16),
        "g_ff": range_draw(shared_keys[13], (D_MODEL,), 0.4, 1.6).astype(jnp.bfloat16),
        "w_router": gauss_draw(shared_keys[14], (D_MODEL, EXPERTS), D_MODEL ** -0.5).astype(jnp.bfloat16),
        "w_gate": gauss_draw(shared_keys[15], (EXPERTS, D_MODEL, FFN_DIM), D_MODEL ** -0.5).astype(jnp.bfloat16),
        "w_up": gauss_draw(shared_keys[16], (EXPERTS, D_MODEL, FFN_DIM), D_MODEL ** -0.5).astype(jnp.bfloat16),
        "w_down": gauss_draw(shared_keys[17], (EXPERTS, FFN_DIM, D_MODEL), EXPERTS * (TOP_K * FFN_DIM) ** -0.5).astype(jnp.bfloat16),
    }


def rms_norm(tensor_in, gain_vec):
    in_f32 = tensor_in.astype(jnp.float32)
    return in_f32 * lax.rsqrt(jnp.mean(in_f32 * in_f32, axis=-1, keepdims=True) + EPSILON) * gain_vec.astype(jnp.float32)


def reference(x_steps, conv_state, ssm_state, expert_ids, g_in, w_in, conv_w, conv_b, w_xp, g_dt, g_b, g_c, w_dt, b_dt, a_log, d_skip, w_out, g_ff, w_router, w_gate, w_up, w_down):
    a_mat = -jnp.exp(a_log)
    w_in_flat = w_in.reshape(D_MODEL, 2 * INNER)

    def expert_body(moe_acc, expert_w):
        w_gate_e, w_up_e, w_down_e, coef_e, moe_in = expert_w
        gate_h = jnp.dot(moe_in, w_gate_e, preferred_element_type=jnp.float32)
        up_h = jnp.dot(moe_in, w_up_e, preferred_element_type=jnp.float32)
        hidden = (jax.nn.silu(gate_h) * up_h).astype(jnp.bfloat16)
        return moe_acc + coef_e[:, None] * jnp.dot(hidden, w_down_e, preferred_element_type=jnp.float32), None

    def one_step(state_pair, step_in):
        conv_st, ssm_st = state_pair
        x_now, ids_now = step_in
        norm_in = rms_norm(x_now, g_in).astype(jnp.bfloat16)
        proj_xz = jnp.dot(norm_in, w_in_flat, preferred_element_type=jnp.float32).astype(jnp.bfloat16).reshape(BATCH_SIZE, 2, INNER)
        x_inner = proj_xz[:, 0]
        z_gate = proj_xz[:, 1]
        conv_win = jnp.concatenate([conv_st, x_inner[:, :, None]], axis=2)
        conv_pre = jnp.sum(conv_win.astype(jnp.float32) * conv_w.astype(jnp.float32)[None], axis=2) + conv_b.astype(jnp.float32)[None]
        x_conv = jax.nn.silu(conv_pre).astype(jnp.bfloat16)
        proj_sum = jnp.dot(x_conv, w_xp, preferred_element_type=jnp.float32)
        dt_low = rms_norm(proj_sum[:, :DT_RANK], g_dt)
        b_vec = rms_norm(proj_sum[:, DT_RANK:DT_RANK + STATE_DIM], g_b)
        c_vec = rms_norm(proj_sum[:, DT_RANK + STATE_DIM:], g_c)
        delta_t = jax.nn.softplus(jnp.dot(dt_low.astype(jnp.bfloat16), w_dt, preferred_element_type=jnp.float32) + b_dt.astype(jnp.float32)[None])
        xc_f32 = x_conv.astype(jnp.float32)
        new_ssm = jnp.exp(delta_t[:, :, None] * a_mat[None]) * ssm_st + (delta_t * xc_f32)[:, :, None] * b_vec[:, None, :]
        y_gated = (jnp.sum(new_ssm * c_vec[:, None, :], axis=2) + d_skip[None] * xc_f32) * jax.nn.silu(z_gate.astype(jnp.float32))
        mix_out = jnp.dot(y_gated.astype(jnp.bfloat16), w_out, preferred_element_type=jnp.float32)
        resid_mid = (x_now.astype(jnp.float32) + mix_out).astype(jnp.bfloat16)
        moe_in = rms_norm(resid_mid, g_ff).astype(jnp.bfloat16)
        route_prob = jax.nn.softmax(jnp.dot(moe_in, w_router, preferred_element_type=jnp.float32), axis=-1)
        pick_count = jnp.sum((ids_now[:, :, None] == jnp.arange(EXPERTS)[None, None, :]).astype(jnp.float32), axis=1)
        combine_w = route_prob * pick_count
        moe_stack = jnp.broadcast_to(moe_in[None], (EXPERTS, BATCH_SIZE, D_MODEL))
        moe_out, _ = lax.scan(expert_body, jnp.zeros((BATCH_SIZE, D_MODEL), jnp.float32), (w_gate, w_up, w_down, combine_w.T, moe_stack))
        out_now = (resid_mid.astype(jnp.float32) + moe_out).astype(jnp.bfloat16)
        return (conv_win[:, :, 1:], new_ssm), out_now

    final_pair, y_steps = lax.scan(one_step, (conv_state, ssm_state), (x_steps, expert_ids))
    return y_steps, final_pair[0], final_pair[1]
```

```python
import functools

import jax
import jax.numpy as jnp
from jax import lax
from jax.experimental import pallas as pl
from jax.experimental.pallas import tpu as pltpu
from jax.sharding import PartitionSpec as P

EPSILON = 1e-6
LOG2E = 1.4426950408889634
MESH = pl.DeviceIdType.MESH
BF = jnp.bfloat16
F32 = jnp.float32
NT = (((1,), (1,)), ((), ()))


def sigmoid(v):
    return 1.0 / (1.0 + jnp.exp(-v))


def layer_kernel(cfg, x_hbm, conv_hbm, ssm_hbm, ids_ref, vec_ref, win_ref, convw_ref, wxpt_ref, wdt_ref, alogt_ref, wout_ref, wrt_ref,
                 wg_hbm, wu_hbm, wd_hbm, y_hbm, convo_hbm, ssmo_hbm,
                 xv, seq, hst, wg, wu, wd, winp, w2t, wdt2, a2, nbuf, zbuf, xcb, idsb, ppk, prx, ptx, prs, pn, delta, dxb, ygb,
                 ypart, yrx, ytx1, ytxd, ytx2, yrx1, yrxd, yrx2, opart, orx, otx1, otxd, otx2, orx1, orxd, orx2,
                 ubuf, pwb, mfull, yfull, hid, lsem, ssem, rsem):
    S, Bt, D, C, N, R, E, F = cfg["S"], cfg["B"], cfg["D"], cfg["C"], cfg["N"], cfg["R"], cfg["E"], cfg["F"]
    chips = cfg["chips"]
    half, quarter = Bt // 2, Bt // 8
    eighth = quarter // 2
    phalf, pquart = Bt // 4, Bt // 16

    t = lax.axis_index("tp")
    q = t // 2
    c = t % 2
    dev = lambda chip, core: (chip % chips) * 2 + core
    right, left, opp, partner = dev(q + 1, c), dev(q + chips - 1, c), dev(q + 2, c), q * 2 + (1 - c)
    q_r, q_l, q_o = (q + 1) % chips, (q + chips - 1) % chips, (q + 2) % chips

    lcount = [0]

    def local(src, dst):
        cp = pltpu.make_async_copy(src, dst, lsem.at[lcount[0]])
        lcount[0] += 1
        cp.start()
        return cp

    ld_x = [local(x_hbm.at[s], xv.at[s]) for s in range(S)]
    ld_conv = local(conv_hbm, seq.at[pl.ds(0, 3)])
    ld_h = [local(ssm_hbm.at[:, n, :], hst.at[n]) for n in range(N)]
    ld_w = [local(wg_hbm, wg), local(wu_hbm, wu), local(wd_hbm, wd)]

    barrier = pltpu.get_barrier_semaphore()
    for peer in (partner, right, left, opp):
        pl.semaphore_signal(barrier, inc=1, device_id={"tp": peer}, device_id_type=MESH)

    keys = {}

    def remote(key, src, dst, peer):
        i = keys.setdefault(key, len(keys))
        cp = pltpu.make_async_remote_copy(src_ref=src, dst_ref=dst, send_sem=ssem.at[i], recv_sem=rsem.at[i],
                                          device_id={"tp": peer}, device_id_type=MESH)
        cp.start()
        live[key] = cp

    live = {}

    def got(*ks):
        for k in ks:
            live[k].wait_recv()

    g_in = vec_ref[0:1, :]
    g_ff = vec_ref[1:2, :]
    g_p = vec_ref[2:3, 0:C]
    conv_b = vec_ref[2:3, C:2 * C]
    b_dt = vec_ref[2:3, 2 * C:3 * C]
    d_skip = vec_ref[2:3, 3 * C:4 * C]

    ri = lax.broadcasted_iota(jnp.int32, (2 * C, 2 * C), 0)
    ci = lax.broadcasted_iota(jnp.int32, (2 * C, 2 * C), 1)
    src_row = jnp.where(ri < C, 2 * ri, 2 * (ri - C) + 1)
    perm = (ci == src_row).astype(BF)
    for blk in range(D // C):
        deint = jnp.dot(perm, win_ref[pl.ds(blk * 2 * C, 2 * C), :], preferred_element_type=F32).astype(BF)
        winp[pl.ds(blk * C, C), 0:C] = deint[0:C]
        winp[pl.ds(blk * C, C), C:2 * C] = deint[C:2 * C]
    PW = R + 2 * N
    w2t[...] = jnp.zeros_like(w2t)
    w2t[0:PW, 0:C] = wxpt_ref[...]
    w2t[PW:2 * PW, C:2 * C] = wxpt_ref[...]
    wdt2[...] = jnp.zeros_like(wdt2)
    wdt2[0:R, 0:C] = wdt_ref[...]
    wdt2[PW:PW + R, C:2 * C] = wdt_ref[...]
    a2[...] = -jnp.exp(alogt_ref[...]) * LOG2E
    for s in range(S):
        row = ids_ref[s].astype(F32)
        idsb[s] = jnp.transpose(jnp.broadcast_to(row, (C, Bt)))

    def rms_rows(v, gain):
        return v * lax.rsqrt(jnp.mean(v * v, axis=-1, keepdims=True) + EPSILON) * gain

    def stage_a(s):
        ld_x[s].wait()
        if s == 0:
            ld_conv.wait()

        def norm_body(i, _):
            rows = pl.ds(pl.multiple_of(i * 64, 64), 64)
            nbuf[rows, :] = rms_rows(xv[s, rows, :].astype(F32), g_in).astype(BF)
            return 0

        lax.fori_loop(0, Bt // 64, norm_body, 0)

        def proj_body(i, _):
            rows = pl.ds(pl.multiple_of(i * 128, 128), 128)
            xz = jnp.dot(nbuf[rows, :], winp[...], preferred_element_type=F32).astype(BF)
            seq[3 + s, rows, :] = xz[:, 0:C]
            zbuf[s, rows, :] = xz[:, C:2 * C]
            acc = xz[:, 0:C].astype(F32) * convw_ref[3:4, :].astype(F32) + conv_b
            for j in range(3):
                acc = acc + seq[s + j, rows, :].astype(F32) * convw_ref[j:j + 1, :].astype(F32)
            xcb[s, rows, :] = (acc * sigmoid(acc)).astype(BF)
            return 0

        lax.fori_loop(0, Bt // 128, proj_body, 0)
        xc2 = jnp.concatenate([xcb[s, 0:half, :], xcb[s, half:Bt, :]], axis=1)
        ppk[s] = lax.dot_general(xc2, w2t[...], NT, preferred_element_type=F32)
        if s == 0:
            pl.semaphore_wait(barrier, 4)
        mine = pl.ds(pl.multiple_of((1 - c) * phalf, phalf), phalf)
        remote(("p0", s), ppk.at[s, mine], prx.at[s], partner)

    def p_rows(j):
        return pl.ds(pl.multiple_of(c * phalf + j * pquart, pquart), pquart)

    def stage_p1(s):
        got(("p0", s))
        ptx[s] = ppk[s, pl.ds(pl.multiple_of(c * phalf, phalf), phalf), :] + prx[s]
        for k, (peer, j) in enumerate(((right, q_r), (left, q_l), (opp, q_o))):
            src = ptx.at[s, pl.ds(pl.multiple_of(j * pquart, pquart), pquart)]
            remote(("p1", s, k), src, prs.at[s, k], peer)

    def stage_p2(s):
        got(*[("p1", s, k) for k in range(3)])
        v = ptx[s, pl.ds(pl.multiple_of(q * pquart, pquart), pquart), :] + prs[s, 0] + prs[s, 1] + prs[s, 2]
        lane = lax.broadcasted_iota(jnp.int32, v.shape, 1)
        sq = v * v
        scale = jnp.zeros_like(v)
        for base in (0, PW):
            for lo, width in ((0, R), (R, N), (R + N, N)):
                inside = (lane >= base + lo) & (lane < base + lo + width)
                ms = jnp.sum(jnp.where(inside, sq, 0.0), axis=-1, keepdims=True) * (1.0 / width)
                scale = jnp.where(inside, lax.rsqrt(ms + EPSILON), scale)
        pn[s, p_rows(q), :] = v * scale * g_p
        for k, peer in enumerate((right, left, opp)):
            remote(("p2", s, k), pn.at[s, p_rows(q)], pn.at[s, p_rows(q)], peer)

    def stage_p3(s):
        got(*[("p2", s, k) for k in range(3)])
        own = pl.ds(pl.multiple_of(c * phalf, phalf), phalf)
        remote(("p3", s), pn.at[s, own], pn.at[s, own], partner)

    def stage_ssm(s):
        got(("p3", s))
        if s == 0:
            for cp in ld_h:
                cp.wait()
        raw = jnp.dot(pn[s].astype(BF), wdt2[...], preferred_element_type=F32)
        for hf in range(2):
            v = raw[:, hf * C:(hf + 1) * C] + b_dt
            rows = pl.ds(hf * half, half)
            dl = jnp.maximum(v, 0.0) + jnp.log1p(jnp.exp(-jnp.abs(v)))
            delta[rows, :] = dl
            dxb[rows, :] = dl * xcb[s, rows, :].astype(F32)
        blk = 32

        def body(i, _):
            pb = pn[s, pl.ds(pl.multiple_of(i * blk, blk), blk), :]
            for hf in range(2):
                rows = pl.ds(pl.multiple_of(hf * half + i * blk, blk), blk)
                d = delta[rows, :]
                dx = dxb[rows, :]
                acc = d_skip * xcb[s, rows, :].astype(F32)
                for n in range(N):
                    b_col = hf * PW + R + n
                    c_col = b_col + N
                    bb = jnp.broadcast_to(pb[:, b_col:b_col + 1], (blk, C))
                    cc = jnp.broadcast_to(pb[:, c_col:c_col + 1], (blk, C))
                    hn = jnp.exp2(d * a2[n:n + 1, :]) * hst[n, rows, :] + dx * bb
                    hst[n, rows, :] = hn
                    acc = acc + hn * cc
                zf = zbuf[s, rows, :].astype(F32)
                ygb[rows, :] = (acc * (zf * sigmoid(zf))).astype(BF)
            return 0

        lax.fori_loop(0, half // blk, body, 0)

        def out_body(i, _):
            rows = pl.ds(pl.multiple_of(i * 128, 128), 128)
            ypart[s, rows, :] = jnp.dot(ygb[rows, :], wout_ref[...], preferred_element_type=F32).astype(BF)
            return 0

        lax.fori_loop(0, Bt // 128, out_body, 0)
        rs0("y", s)

    bufs = {"y": (ypart, yrx, ytx1, ytxd, ytx2, yrx1, yrxd, yrx2), "o": (opart, orx, otx1, otxd, otx2, orx1, orxd, orx2)}

    def rs0(w, s):
        part, prx_ = bufs[w][0:2]
        src = pl.ds(pl.multiple_of((1 - c) * half, half), half)
        remote((w, 0, s), part.at[s, src], prx_.at[s], partner)

    def chip_sum(w, s, j, hv):
        part, prx_ = bufs[w][0:2]
        a = part[s, pl.ds(pl.multiple_of(c * half + j * quarter + hv * eighth, eighth), eighth), :].astype(F32)
        b = prx_[s, pl.ds(pl.multiple_of(j * quarter + hv * eighth, eighth), eighth), :].astype(F32)
        return a + b

    def rs1(w, s):
        _, _, tx1, txd, _, rx1, rxd, _ = bufs[w]
        got((w, 0, s))
        tx1[s, 0] = chip_sum(w, s, q_o, 0).astype(BF)
        remote((w, 1, s, 0), tx1.at[s, 0], rx1.at[s, 0], right)
        tx1[s, 1] = chip_sum(w, s, q_o, 1).astype(BF)
        remote((w, 1, s, 1), tx1.at[s, 1], rx1.at[s, 1], left)
        txd[s, 0] = chip_sum(w, s, q_r, 1).astype(BF)
        remote((w, 2, s, 0), txd.at[s, 0], rxd.at[s, 0], right)
        txd[s, 1] = chip_sum(w, s, q_l, 0).astype(BF)
        remote((w, 2, s, 1), txd.at[s, 1], rxd.at[s, 1], left)

    def rs2(w, s):
        _, _, _, _, tx2, rx1, _, rx2 = bufs[w]
        got((w, 1, s, 0))
        tx2[s, 0] = (chip_sum(w, s, q_r, 0) + rx1[s, 0].astype(F32)).astype(BF)
        remote((w, 3, s, 0), tx2.at[s, 0], rx2.at[s, 0], right)
        got((w, 1, s, 1))
        tx2[s, 1] = (chip_sum(w, s, q_l, 1) + rx1[s, 1].astype(F32)).astype(BF)
        remote((w, 3, s, 1), tx2.at[s, 1], rx2.at[s, 1], left)

    def rs3(w, s):
        _, _, _, _, _, _, rxd, rx2 = bufs[w]
        got((w, 2, s, 0), (w, 2, s, 1), (w, 3, s, 0), (w, 3, s, 1))
        lo = chip_sum(w, s, q, 0) + rx2[s, 0].astype(F32) + rxd[s, 1].astype(F32)
        hi = chip_sum(w, s, q, 1) + rx2[s, 1].astype(F32) + rxd[s, 0].astype(F32)
        return lo, hi

    def rows_of(j, hv=None):
        if hv is None:
            return pl.ds(pl.multiple_of(c * half + j * quarter, quarter), quarter)
        return pl.ds(pl.multiple_of(c * half + j * quarter + hv * eighth, eighth), eighth)

    def ag1(w, buf, s):
        own = buf.at[s, rows_of(q)]
        remote((w, 0, s, 0), own, own, right)
        remote((w, 0, s, 1), own, own, left)
        remote((w, 1, s, 0), own, own, partner)

    def ag2(w, buf, s):
        got((w, 0, s, 0))
        fwd = buf.at[s, rows_of(q_l, 0)]
        remote((w, 2, s, 0), fwd, fwd, right)
        got((w, 0, s, 1))
        fwd = buf.at[s, rows_of(q_r, 1)]
        remote((w, 2, s, 1), fwd, fwd, left)
        for k, j in enumerate((q_l, q_r)):
            sh = buf.at[s, rows_of(j)]
            remote((w, 1, s, 1 + k), sh, sh, partner)

    def ag3(w, buf, s):
        got((w, 2, s, 0), (w, 2, s, 1))
        sh = buf.at[s, rows_of(q_o)]
        remote((w, 1, s, 3), sh, sh, partner)

    def ag4(w, s):
        got(*[(w, 1, s, k) for k in range(4)])

    def y3(s):
        sums = rs3("y", s)
        for hv in range(2):
            rows = rows_of(q, hv)
            loc = pl.ds(hv * eighth, eighth)
            u = (xv[s, rows, :].astype(F32) + sums[hv]).astype(BF)
            ubuf[s, loc, :] = u
            mfull[s, rows, :] = rms_rows(u.astype(F32), g_ff).astype(BF)
        ag1("m", mfull, s)
        logits = lax.dot_general(mfull[s, rows_of(q), :], wrt_ref[...], NT, preferred_element_type=F32)
        ex = jnp.exp(logits - jnp.max(logits, axis=-1, keepdims=True))
        ids = idsb[s, rows_of(q), :][:, 0:E]
        pick = jnp.where(lax.broadcasted_iota(jnp.int32, ex.shape, 1).astype(F32) == ids, ex, 0.0)
        prob = jnp.sum(pick, axis=-1, keepdims=True) / jnp.sum(ex, axis=-1, keepdims=True)
        pwb[s] = jnp.broadcast_to(prob, (quarter, C))

    def o3(s):
        sums = rs3("o", s)
        for hv in range(2):
            rows = rows_of(q, hv)
            loc = pl.ds(hv * eighth, eighth)
            pw = pwb[s, loc, :][:, 0:1]
            yfull[s, rows, :] = (ubuf[s, loc, :].astype(F32) + pw * sums[hv]).astype(BF)
        ag1("z", yfull, s)

    def moe_part(s, lo, hi):
        def body(e, _):
            m = mfull[s]
            gate = jnp.dot(m, wg[e], preferred_element_type=F32)
            up = jnp.dot(m, wu[e], preferred_element_type=F32)
            act = gate * sigmoid(gate) * up
            keep = idsb[s] == e.astype(F32)
            cols = pl.ds(pl.multiple_of(e * F, F), F)
            hid[:, cols] = jnp.concatenate([jnp.where(keep, act[:, k * C:(k + 1) * C], 0.0) for k in range(F // C)], axis=1).astype(BF)
            return 0

        lax.fori_loop(lo, hi, body, 0)

    def moe_down(s):
        def body(i, _):
            rows = pl.ds(pl.multiple_of(i * 256, 256), 256)
            opart[s, rows, :] = jnp.dot(hid[rows, :], wd[...], preferred_element_type=F32).astype(BF)
            return 0

        lax.fori_loop(0, Bt // 256, body, 0)
        rs0("o", s)

    st_y = []

    def y_out(s):
        ag4("z", s)
        st_y.append(local(yfull.at[s], y_hbm.at[s]))

    acts = {
        "A": stage_a, "p1": stage_p1, "p2": stage_p2, "p3": stage_p3, "S": stage_ssm,
        "y1": lambda s: rs1("y", s), "y2": lambda s: rs2("y", s), "y3": y3,
        "m2": lambda s: ag2("m", mfull, s), "m3": lambda s: ag3("m", mfull, s), "m4": lambda s: ag4("m", s),
        "o1": lambda s: rs1("o", s), "o2": lambda s: rs2("o", s), "o3": o3,
        "z2": lambda s: ag2("z", yfull, s), "z3": lambda s: ag3("z", yfull, s), "z4": y_out, "D": moe_down,
    }
    for k in range(4):
        acts["M%d" % k] = functools.partial(lambda k, s: moe_part(s, k * (E // 4), (k + 1) * (E // 4)), k)

    st_state = []

    def run(*plan):
        for item in plan:
            name, s = item.split(".")
            acts[name](int(s))

    run("A.0", "A.1", "p1.0", "A.2", "p1.1", "A.3", "p2.0", "p1.2", "p2.1", "p3.0", "p1.3", "p2.2", "p3.1", "S.0", "p2.3", "p3.2", "S.1", "y1.0", "p3.3", "S.2", "y2.0", "y1.1", "S.3")
    st_state.append(local(seq.at[pl.ds(S, 3)], convo_hbm))
    for n in range(N):
        st_state.append(local(hst.at[n], ssmo_hbm.at[:, n, :]))
    run("y3.0", "y2.1", "y1.2", "m2.0", "y3.1", "y2.2", "y1.3", "m3.0", "m2.1", "y3.2", "y2.3", "m4.0")
    for cp in ld_w:
        cp.wait()
    run("M0.0", "m3.1", "y3.3", "M1.0", "m2.2", "M2.0", "m3.2", "m2.3", "M3.0", "m3.3", "D.0")
    run("m4.1", "M0.1", "o1.0", "M1.1", "o2.0", "M2.1", "o3.0", "M3.1", "z2.0", "D.1")
    run("m4.2", "M0.2", "z3.0", "o1.1", "M1.2", "z4.0", "o2.1", "M2.2", "o3.1", "M3.2", "z2.1", "D.2")
    run("m4.3", "M0.3", "z3.1", "o1.2", "M1.3", "z4.1", "o2.2", "M2.3", "o3.2", "M3.3", "z2.2", "D.3")
    run("z3.2", "o1.3", "z4.2", "o2.3", "o3.3", "z2.3", "z3.3", "z4.3")
    for cp in live.values():
        cp.wait_send()
    for cp in st_state + st_y:
        cp.wait()


def solution(mesh):
    act_spec = P(None, "dp", None)
    state_spec = P("dp", "tp", None)
    in_specs = (act_spec, state_spec, state_spec, act_spec, P(None), P(None, None, "tp"), P("tp", None), P("tp"), P("tp", None), P(None), P(None), P(None), P(None, "tp"), P("tp"), P("tp", None), P("tp"), P("tp", None), P(None), P(None, None), P(None, None, "tp"), P(None, None, "tp"), P(None, "tp", None))
    out_specs = (act_spec, state_spec, state_spec)
    chips = mesh.shape["tp"] // 2
    assert chips == 4

    def layer_steps(x_steps, conv_state, ssm_state, expert_ids, g_in, w_in, conv_w, conv_b, w_xp, g_dt, g_b, g_c, w_dt, b_dt, a_log, d_skip, w_out, g_ff, w_router, w_gate, w_up, w_down):
        S, B, D = x_steps.shape
        C = w_in.shape[2]
        R = w_dt.shape[0]
        N = a_log.shape[1]
        E, _, F = w_gate.shape
        assert expert_ids.shape[2] == 1 and D == 4 * C and 2 * (R + 2 * N) == C
        cfg = dict(S=S, B=B, D=D, C=C, N=N, R=R, E=E, F=F, chips=chips)
        f = lambda a: a.astype(F32)
        vec = jnp.concatenate([f(g_in), f(g_ff), f(g_dt), f(g_b), f(g_c), f(g_dt), f(g_b), f(g_c), f(conv_b), f(b_dt), d_skip,
                               jnp.zeros((5 * D,), F32)]).reshape(8, D)
        vm = pl.BlockSpec(memory_space=pltpu.VMEM)
        anym = pl.BlockSpec(memory_space=pl.ANY)
        half, quarter, eighth = B // 2, B // 8, B // 16
        ring = lambda: [
            pltpu.VMEM((S, B, D), BF), pltpu.VMEM((S, half, D), BF),
            pltpu.VMEM((S, 2, eighth, D), BF), pltpu.VMEM((S, 2, eighth, D), BF), pltpu.VMEM((S, 2, eighth, D), BF),
            pltpu.VMEM((S, 2, eighth, D), BF), pltpu.VMEM((S, 2, eighth, D), BF), pltpu.VMEM((S, 2, eighth, D), BF)]
        n_remote = S * (8 + 2 * 7 + 2 * 8)
        scratch = [
            pltpu.VMEM((S, B, D), BF), pltpu.VMEM((3 + S, B, C), BF), pltpu.VMEM((N, B, C), F32),
            pltpu.VMEM((E, D, F), BF), pltpu.VMEM((E, D, F), BF), pltpu.VMEM((E * F, D), BF),
            pltpu.VMEM((D, 2 * C), BF), pltpu.VMEM((C, 2 * C), BF), pltpu.VMEM((C, 2 * C), BF), pltpu.VMEM((N, C), F32),
            pltpu.VMEM((B, D), BF), pltpu.VMEM((S, B, C), BF), pltpu.VMEM((S, B, C), BF), pltpu.VMEM((S, B, C), F32),
            pltpu.VMEM((S, half, C), F32), pltpu.VMEM((S, half // 2, C), F32), pltpu.VMEM((S, half // 2, C), F32),
            pltpu.VMEM((S, 3, B // 16, C), F32), pltpu.VMEM((S, half, C), F32),
            pltpu.VMEM((B, C), F32), pltpu.VMEM((B, C), F32), pltpu.VMEM((B, C), BF),
            *ring(), *ring(),
            pltpu.VMEM((S, quarter, D), BF), pltpu.VMEM((S, quarter, C), F32),
            pltpu.VMEM((S, B, D), BF), pltpu.VMEM((S, B, D), BF), pltpu.VMEM((B, E * F), BF),
            pltpu.SemaphoreType.DMA((2 * S + 2 + 2 * N + 3,)),
            pltpu.SemaphoreType.DMA((n_remote,)), pltpu.SemaphoreType.DMA((n_remote,)),
        ]
        y, conv_o, ssm_o = pl.pallas_call(
            functools.partial(layer_kernel, cfg),
            out_shape=(jax.ShapeDtypeStruct((S, B, D), BF), jax.ShapeDtypeStruct((3, B, C), BF), jax.ShapeDtypeStruct((B, N, C), F32)),
            in_specs=[anym, anym, anym, vm, vm, vm, vm, vm, vm, vm, vm, vm, anym, anym, anym],
            out_specs=(anym, anym, anym),
            scratch_shapes=scratch,
            compiler_params=pltpu.CompilerParams(collective_id=0, has_side_effects=True, vmem_limit_bytes=62 * 1024 * 1024),
            name="layer_steps",
        )(x_steps, conv_state.transpose(2, 0, 1), ssm_state.transpose(0, 2, 1), expert_ids.transpose(0, 2, 1), vec,
          w_in.reshape(2 * D, C), conv_w.T, w_xp.T, w_dt, a_log.T, w_out, w_router.T, w_gate, w_up, w_down.reshape(E * F, D))
        return y, conv_o.transpose(1, 2, 0), ssm_o.transpose(0, 2, 1)

    return jax.shard_map(layer_steps, mesh=mesh, in_specs=in_specs, out_specs=out_specs, check_vma=False)
```

```python
import functools

import jax
import jax.numpy as jnp
from jax import lax
from jax.experimental import pallas as pl
from jax.experimental.pallas import tpu as pltpu
from jax.sharding import PartitionSpec as P

EPSILON = 1e-6
LOG2E = 1.4426950408889634
MESH = pl.DeviceIdType.MESH
BF = jnp.bfloat16
F32 = jnp.float32
NT = (((1,), (1,)), ((), ()))


def silu(v):
    h = 0.5 * v
    return h + h * jnp.tanh(h)


def layer_kernel(cfg, x_hbm, conv_hbm, ssm_hbm, tt_ref, ids_ref, gin_ref, gff_ref, gdt_ref, gb_ref, gc_ref, win_ref, convw_ref, convb_ref,
                 wxpt_ref, wdt_ref, bdt_ref, alogt_ref, dskip_ref, wout_ref, wrt_ref, wg_hbm, wu_hbm, wd_hbm, y_hbm, convo_hbm, ssmo_hbm,
                 xv, cst, seq, hst, wg, wu, wd, wint, ab, cols, gp, nbuf, zbuf, xcb, idsb, rcb, pm, ubig, msort, hbuf, opair,
                 ppk, prx, ptx, prs, pn, delta, dxb, ygb,
                 ypart, yrx, ytx1, ytxd, ytx2, yrx1, yrxd, yrx2, opart, orx, otx1, otxd, otx2, orx1, orxd, orx2,
                 ubuf, pwb, mfull, yfull, lsem, ssem, rsem):
    S, Bt, D, C, N, R, E, F = cfg["S"], cfg["B"], cfg["D"], cfg["C"], cfg["N"], cfg["R"], cfg["E"], cfg["F"]
    chips, T, tiles, slots = cfg["chips"], cfg["T"], cfg["tiles"], cfg["slots"]
    half, quarter = Bt // 2, Bt // 8
    eighth = quarter // 2
    JB = Bt // C
    PH = R

    t = lax.axis_index("tp")
    q = t // 2
    c = t % 2
    dev = lambda chip, core: (chip % chips) * 2 + core
    right, left, opp, partner = dev(q + 1, c), dev(q + chips - 1, c), dev(q + 2, c), q * 2 + (1 - c)
    q_r, q_l, q_o = (q + 1) % chips, (q + chips - 1) % chips, (q + 2) % chips

    lcount = [0]

    def local(src, dst):
        cp = pltpu.make_async_copy(src, dst, lsem.at[lcount[0]])
        lcount[0] += 1
        cp.start()
        return cp

    ld_x = [local(x_hbm.at[s], xv.at[s]) for s in range(S)]
    ld_conv = local(conv_hbm, cst)
    ld_h = [local(ssm_hbm.at[:, n, :], hst.at[n]) for n in range(N)]
    ld_w = [local(wg_hbm, wg), local(wu_hbm, wu), local(wd_hbm, wd)]

    barrier = pltpu.get_barrier_semaphore()
    for peer in (partner, right, left, opp):
        pl.semaphore_signal(barrier, inc=1, device_id={"tp": peer}, device_id_type=MESH)

    keys = {}
    live = {}

    def remote(key, src, dst, peer):
        i = keys.setdefault(key, len(keys))
        cp = pltpu.make_async_remote_copy(src_ref=src, dst_ref=dst, send_sem=ssem.at[i], recv_sem=rsem.at[i],
                                          device_id={"tp": peer}, device_id_type=MESH)
        cp.start()
        live[key] = cp

    def got(*ks):
        for k in ks:
            live[k].wait_recv()

    g_in = gin_ref[...].astype(F32)
    g_ff = gff_ref[...].astype(F32)

    ri = lax.broadcasted_iota(jnp.int32, (2 * C, 2 * C), 0)
    ci = lax.broadcasted_iota(jnp.int32, (2 * C, 2 * C), 1)
    src_row = jnp.where(ri < C, 2 * ri, 2 * (ri - C) + 1)
    perm = (ci == src_row).astype(BF)
    for blk in range(D // C):
        rows = win_ref[pl.ds(blk * 2 * C, 2 * C), :]
        deint = lax.dot_general(rows, perm, (((0,), (1,)), ((), ())), preferred_element_type=F32).astype(BF)
        wint[0:C, pl.ds(blk * C, C)] = deint[:, 0:C]
        wint[C:2 * C, pl.ds(blk * C, C)] = deint[:, C:2 * C]

    def column(row):
        return jnp.transpose(jnp.broadcast_to(row, (C, C)))

    for j in range(4):
        cols[j] = column(convw_ref[j:j + 1, :].astype(F32))
    cols[4] = column(convb_ref[...].astype(F32))
    cols[5] = column(bdt_ref[...].astype(F32))
    cols[6] = column(dskip_ref[...])

    def small_column(ref):
        w = ref.shape[1]
        eye = lax.broadcasted_iota(jnp.int32, (w, w), 0) == lax.broadcasted_iota(jnp.int32, (w, w), 1)
        v = jnp.where(eye, jnp.broadcast_to(ref[...].astype(F32), (w, w)), 0.0)
        return jnp.broadcast_to(jnp.sum(v, axis=1, keepdims=True), (w, C))

    gp[0:R, :] = small_column(gdt_ref)
    gp[R:R + N, :] = small_column(gb_ref)
    gp[R + N:R + 2 * N, :] = small_column(gc_ref)

    def rms_rows(v, gain):
        return v * lax.rsqrt(jnp.mean(v * v, axis=-1, keepdims=True) + EPSILON) * gain

    def conv_in(_):
        ld_conv.wait()
        for k in range(3):
            for j in range(JB):
                blk = cst[k, pl.ds(j * C, C), :].astype(F32)
                seq[k, j] = jnp.transpose(blk).astype(BF)

    def a_in(_):
        for n in range(N):
            ab[n] = column(-jnp.exp(alogt_ref[n:n + 1, :]) * LOG2E)

    def h_flip():
        def body(n, _):
            for j in range(JB):
                rows = pl.ds(j * C, C)
                hst[n, rows, :] = jnp.transpose(hst[n, rows, :])
            return 0

        lax.fori_loop(0, N, body, 0)

    def h_in(_):
        for cp in ld_h:
            cp.wait()
        h_flip()

    st_state = []

    def state_out(_):
        h_flip()
        for n in range(N):
            st_state.append(local(hst.at[n], ssmo_hbm.at[:, n, :]))
        for k in range(3):
            for j in range(JB):
                cst[k, pl.ds(j * C, C), :] = jnp.transpose(seq[S + k, j].astype(F32)).astype(BF)
        st_state.append(local(cst, convo_hbm))

    def route_prep(s):
        row = ids_ref[s].astype(F32)
        idb = jnp.transpose(jnp.broadcast_to(row, (C, Bt)))
        idsb[s] = idb
        lane = lax.broadcasted_iota(jnp.int32, (Bt, C), 1).astype(F32)
        hot = idb == lane
        before = (lax.broadcasted_iota(jnp.int32, (Bt, Bt), 1) < lax.broadcasted_iota(jnp.int32, (Bt, Bt), 0)).astype(BF)
        cum = jnp.dot(before, hot.astype(BF), preferred_element_type=F32)
        off = jnp.dot(jnp.ones((8, Bt), BF), (idb < lane).astype(BF), preferred_element_type=F32)[0:1, :]
        pos = jnp.sum(jnp.where(hot, cum + off, 0.0), axis=1, keepdims=True)
        posb = jnp.broadcast_to(pos, (Bt, C))
        rcb[...] = idb * float(T) + posb
        pos_row = jnp.transpose(posb)[0:1, :]
        pm[s] = (lax.broadcasted_iota(jnp.int32, (Bt, Bt), 0).astype(F32) == pos_row).astype(BF)
        lane_c = lax.broadcasted_iota(jnp.int32, (Bt, T), 1).astype(F32)

        def body(k, _):
            ubig[s, :, pl.ds(pl.multiple_of(k * T, T), T)] = (rcb[...] == lane_c + k.astype(F32) * T).astype(BF)
            return 0

        lax.fori_loop(0, slots, body, 0)

    def stage_a(s):
        ld_x[s].wait()

        def norm_body(i, _):
            rows = pl.ds(pl.multiple_of(i * 64, 64), 64)
            nbuf[rows, :] = rms_rows(xv[s, rows, :].astype(F32), g_in).astype(BF)
            return 0

        lax.fori_loop(0, Bt // 64, norm_body, 0)
        if s == 0:
            conv_in(0)
        for j in range(JB):
            xz = lax.dot_general(wint[...], nbuf[pl.ds(j * C, C), :], NT, preferred_element_type=F32).astype(BF)
            seq[3 + s, j] = xz[0:C]
            zbuf[s, j] = xz[C:2 * C]
            acc = xz[0:C].astype(F32) * cols[3] + cols[4]
            for k in range(3):
                acc = acc + seq[s + k, j].astype(F32) * cols[k]
            xc = silu(acc).astype(BF)
            xcb[s, j] = xc
            ppk[s, j] = jnp.dot(wxpt_ref[...], xc, preferred_element_type=F32)
        if s == 0:
            pl.semaphore_wait(barrier, 4)
        theirs = pl.ds(pl.multiple_of((1 - c) * PH, PH), PH)
        remote(("p0", s), ppk.at[s, :, theirs], prx.at[s], partner)

    own_half = pl.ds(pl.multiple_of(c * PH, PH), PH)

    def stage_p1(s):
        got(("p0", s))
        ptx[s] = ppk[s, :, own_half, :] + prx[s]
        for k, (peer, j) in enumerate(((right, q_r), (left, q_l), (opp, q_o))):
            remote(("p1", s, k), ptx.at[s, j], prs.at[s, k], peer)

    def stage_p2(s):
        got(*[("p1", s, k) for k in range(3)])
        v = ptx[s, q] + prs[s, 0] + prs[s, 1] + prs[s, 2]
        sq = v * v
        sa = jnp.sum(sq[0:N], axis=0, keepdims=True)
        sb = jnp.sum(sq[N:2 * N], axis=0, keepdims=True)
        whole = (sa + sb) * (1.0 / R)
        first = jnp.where(c == 0, whole, sa * (1.0 / N))
        second = jnp.where(c == 0, whole, sb * (1.0 / N))
        gain = gp[own_half, :]
        pn[s, q, pl.ds(pl.multiple_of(c * PH, PH), N), :] = v[0:N] * lax.rsqrt(first + EPSILON) * gain[0:N]
        pn[s, q, pl.ds(pl.multiple_of(c * PH + N, N), N), :] = v[N:2 * N] * lax.rsqrt(second + EPSILON) * gain[N:2 * N]
        for k, peer in enumerate((right, left, opp)):
            sh = pn.at[s, q, own_half]
            remote(("p2", s, k), sh, sh, peer)

    def stage_p3(s):
        got(*[("p2", s, k) for k in range(3)])
        sh = pn.at[s, :, own_half]
        remote(("p3", s), sh, sh, partner)

    def stage_ssm(s):
        got(("p3", s))
        blk = 64
        for j in range(JB):
            v = lax.dot_general(wdt_ref[...], pn[s, j, 0:R, :].astype(BF), (((0,), (0,)), ((), ())), preferred_element_type=F32) + cols[5]
            dl = jnp.maximum(v, 0.0) + jnp.log1p(jnp.exp(-jnp.abs(v)))
            delta[j] = dl
            dxb[j] = dl * xcb[s, j].astype(F32)

        def body(i, _):
            j = i // (C // blk)
            r0 = (i % (C // blk)) * blk
            rows = pl.ds(pl.multiple_of(r0, blk), blk)
            hrows = pl.ds(pl.multiple_of(j * C + r0, blk), blk)
            d = delta[j, rows, :]
            dx = dxb[j, rows, :]
            acc = cols[6, rows, :] * xcb[s, j, rows, :].astype(F32)
            for n in range(N):
                bb = pn[s, j, R + n:R + n + 1, :]
                cc = pn[s, j, R + N + n:R + N + n + 1, :]
                hn = jnp.exp2(d * ab[n, rows, :]) * hst[n, hrows, :] + dx * bb
                hst[n, hrows, :] = hn
                acc = acc + hn * cc
            ygb[j, rows, :] = (acc * silu(zbuf[s, j, rows, :].astype(F32))).astype(BF)
            return 0

        lax.fori_loop(0, JB * (C // blk), body, 0)
        for j in range(JB):
            y = lax.dot_general(ygb[j], wout_ref[...], (((0,), (0,)), ((), ())), preferred_element_type=F32)
            ypart[s, pl.ds(j * C, C), :] = y.astype(BF)
        rs0("y", s)

    bufs = {"y": (ypart, yrx, ytx1, ytxd, ytx2, yrx1, yrxd, yrx2), "o": (opart, orx, otx1, otxd, otx2, orx1, orxd, orx2)}

    def rs0(w, s):
        part, prx_ = bufs[w][0:2]
        src = pl.ds(pl.multiple_of((1 - c) * half, half), half)
        remote((w, 0, s), part.at[s, src], prx_.at[s], partner)

    def chip_sum(w, s, j, hv):
        part, prx_ = bufs[w][0:2]
        a = part[s, pl.ds(pl.multiple_of(c * half + j * quarter + hv * eighth, eighth), eighth), :].astype(F32)
        b = prx_[s, pl.ds(pl.multiple_of(j * quarter + hv * eighth, eighth), eighth), :].astype(F32)
        return a + b

    def rs1(w, s):
        _, _, tx1, txd, _, rx1, rxd, _ = bufs[w]
        got((w, 0, s))
        tx1[s, 0] = chip_sum(w, s, q_o, 0).astype(BF)
        remote((w, 1, s, 0), tx1.at[s, 0], rx1.at[s, 0], right)
        tx1[s, 1] = chip_sum(w, s, q_o, 1).astype(BF)
        remote((w, 1, s, 1), tx1.at[s, 1], rx1.at[s, 1], left)
        txd[s, 0] = chip_sum(w, s, q_r, 1).astype(BF)
        remote((w, 2, s, 0), txd.at[s, 0], rxd.at[s, 0], right)
        txd[s, 1] = chip_sum(w, s, q_l, 0).astype(BF)
        remote((w, 2, s, 1), txd.at[s, 1], rxd.at[s, 1], left)

    def rs2(w, s):
        _, _, _, _, tx2, rx1, _, rx2 = bufs[w]
        got((w, 1, s, 0))
        tx2[s, 0] = (chip_sum(w, s, q_r, 0) + rx1[s, 0].astype(F32)).astype(BF)
        remote((w, 3, s, 0), tx2.at[s, 0], rx2.at[s, 0], right)
        got((w, 1, s, 1))
        tx2[s, 1] = (chip_sum(w, s, q_l, 1) + rx1[s, 1].astype(F32)).astype(BF)
        remote((w, 3, s, 1), tx2.at[s, 1], rx2.at[s, 1], left)

    def rs3(w, s):
        _, _, _, _, _, _, rxd, rx2 = bufs[w]
        got((w, 2, s, 0), (w, 2, s, 1), (w, 3, s, 0), (w, 3, s, 1))
        lo = chip_sum(w, s, q, 0) + rx2[s, 0].astype(F32) + rxd[s, 1].astype(F32)
        hi = chip_sum(w, s, q, 1) + rx2[s, 1].astype(F32) + rxd[s, 0].astype(F32)
        return lo, hi

    def rows_of(j, hv=None):
        if hv is None:
            return pl.ds(pl.multiple_of(c * half + j * quarter, quarter), quarter)
        return pl.ds(pl.multiple_of(c * half + j * quarter + hv * eighth, eighth), eighth)

    def ag1(w, buf, s):
        own = buf.at[s, rows_of(q)]
        remote((w, 0, s, 0), own, own, right)
        remote((w, 0, s, 1), own, own, left)
        remote((w, 1, s, 0), own, own, partner)

    def ag2(w, buf, s):
        got((w, 0, s, 0))
        fwd = buf.at[s, rows_of(q_l, 0)]
        remote((w, 2, s, 0), fwd, fwd, right)
        got((w, 0, s, 1))
        fwd = buf.at[s, rows_of(q_r, 1)]
        remote((w, 2, s, 1), fwd, fwd, left)
        for k, j in enumerate((q_l, q_r)):
            sh = buf.at[s, rows_of(j)]
            remote((w, 1, s, 1 + k), sh, sh, partner)

    def ag3(w, buf, s):
        got((w, 2, s, 0), (w, 2, s, 1))
        sh = buf.at[s, rows_of(q_o)]
        remote((w, 1, s, 3), sh, sh, partner)

    def ag4(w, s):
        got(*[(w, 1, s, k) for k in range(4)])

    def y3(s):
        sums = rs3("y", s)
        for hv in range(2):
            rows = rows_of(q, hv)
            loc = pl.ds(hv * eighth, eighth)
            u = (xv[s, rows, :].astype(F32) + sums[hv]).astype(BF)
            ubuf[s, loc, :] = u
            mfull[s, rows, :] = rms_rows(u.astype(F32), g_ff).astype(BF)
        ag1("m", mfull, s)
        logits = lax.dot_general(mfull[s, rows_of(q), :], wrt_ref[...], NT, preferred_element_type=F32)
        ex = jnp.exp(logits - jnp.max(logits, axis=-1, keepdims=True))
        ids = idsb[s, rows_of(q), :][:, 0:E]
        pick = jnp.where(lax.broadcasted_iota(jnp.int32, ex.shape, 1).astype(F32) == ids, ex, 0.0)
        prob = jnp.sum(pick, axis=-1, keepdims=True) / jnp.sum(ex, axis=-1, keepdims=True)
        pwb[s] = jnp.broadcast_to(prob, (quarter, C))

    def o3(s):
        sums = rs3("o", s)
        for hv in range(2):
            rows = rows_of(q, hv)
            loc = pl.ds(hv * eighth, eighth)
            pw = pwb[s, loc, :][:, 0:1]
            yfull[s, rows, :] = (ubuf[s, loc, :].astype(F32) + pw * sums[hv]).astype(BF)
        ag1("z", yfull, s)

    group = -(-slots // 4)

    def moe_part(s, part):
        if part == 0:
            msort[...] = jnp.dot(pm[s], mfull[s], preferred_element_type=F32).astype(BF).reshape(tiles, T, D)
        picks = []
        for k in range(part * group, min(slots, (part + 1) * group)):
            tile = tt_ref[s, k]
            picks.append((k, tile, jnp.clip(k - tile, 0, E - 1)))
        for k, tile, e in picks:
            lhs = msort[tile]
            gate = jnp.dot(lhs, wg[e], preferred_element_type=F32)
            up = jnp.dot(lhs, wu[e], preferred_element_type=F32)
            hbuf[k - part * group] = (silu(gate) * up).astype(BF)
        for k, tile, e in picks:
            opair[k * T:(k + 1) * T, :] = jnp.dot(hbuf[k - part * group], wd[e], preferred_element_type=F32).astype(BF)

    def moe_down(s):
        for i in range(Bt // 256):
            rows = pl.ds(i * 256, 256)
            opart[s, rows, :] = jnp.dot(ubig[s, rows, :], opair[...], preferred_element_type=F32).astype(BF)
        rs0("o", s)

    st_y = []

    def y_out(s):
        ag4("z", s)
        st_y.append(local(yfull.at[s], y_hbm.at[s]))

    acts = {
        "A": stage_a, "p1": stage_p1, "p2": stage_p2, "p3": stage_p3, "S": stage_ssm,
        "y1": lambda s: rs1("y", s), "y2": lambda s: rs2("y", s), "y3": y3,
        "m2": lambda s: ag2("m", mfull, s), "m3": lambda s: ag3("m", mfull, s), "m4": lambda s: ag4("m", s),
        "o1": lambda s: rs1("o", s), "o2": lambda s: rs2("o", s), "o3": o3,
        "z2": lambda s: ag2("z", yfull, s), "z3": lambda s: ag3("z", yfull, s), "z4": y_out, "D": moe_down,
        "W": route_prep, "HI": h_in, "AI": a_in, "SO": state_out,
    }
    for k in range(4):
        acts["M%d" % k] = functools.partial(lambda k, s: moe_part(s, k), k)

    def run(*plan):
        for item in plan:
            name, s = item.split(".")
            acts[name](int(s))

    run("A.0", "A.1", "p1.0", "A.2", "p1.1", "A.3", "p1.2", "p2.0", "AI.0", "p1.3", "p2.1", "HI.0", "p3.0", "p2.2", "W.0", "p3.1", "p2.3")
    run("S.0", "p3.2", "S.1", "y1.0", "p3.3", "S.2", "y1.1", "y2.0", "S.3", "y1.2", "y2.1", "y3.0", "W.1")
    run("y1.3", "y2.2", "y3.1", "m2.0", "W.2", "y2.3", "y3.2", "m2.1", "m3.0", "SO.0", "W.3", "m4.0")
    for cp in ld_w:
        cp.wait()
    run("M0.0", "y3.3", "M1.0", "m3.1", "m2.2", "M2.0", "M3.0", "m2.3", "m3.2", "D.0")
    run("m4.1", "M0.1", "m3.3", "M1.1", "o1.0", "M2.1", "M3.1", "o2.0", "D.1")
    run("m4.2", "M0.2", "o3.0", "M1.2", "o1.1", "M2.2", "z2.0", "M3.2", "o2.1", "D.2")
    run("m4.3", "M0.3", "z3.0", "o3.1", "M1.3", "o1.2", "M2.3", "z4.0", "z2.1", "M3.3", "o2.2", "D.3")
    run("z3.1", "o3.2", "o1.3", "z4.1", "z2.2", "o2.3", "z3.2", "o3.3", "z4.2", "z2.3", "z3.3", "z4.3")
    for cp in live.values():
        cp.wait_send()
    for cp in st_state + st_y:
        cp.wait()


def solution(mesh):
    act_spec = P(None, "dp", None)
    state_spec = P("dp", "tp", None)
    in_specs = (act_spec, state_spec, state_spec, act_spec, P(None), P(None, None, "tp"), P("tp", None), P("tp"), P("tp", None), P(None), P(None), P(None), P(None, "tp"), P("tp"), P("tp", None), P("tp"), P("tp", None), P(None), P(None, None), P(None, None, "tp"), P(None, None, "tp"), P(None, "tp", None))
    out_specs = (act_spec, state_spec, state_spec)
    chips = mesh.shape["tp"] // 2
    assert chips == 4

    def layer_steps(x_steps, conv_state, ssm_state, expert_ids, g_in, w_in, conv_w, conv_b, w_xp, g_dt, g_b, g_c, w_dt, b_dt, a_log, d_skip, w_out, g_ff, w_router, w_gate, w_up, w_down):
        S, B, D = x_steps.shape
        C = w_in.shape[2]
        R = w_dt.shape[0]
        N = a_log.shape[1]
        E, _, F = w_gate.shape
        assert expert_ids.shape[2] == 1 and B == 4 * C and R == 2 * N
        T = 128
        tiles = B // T
        slots = E + tiles - 1
        cfg = dict(S=S, B=B, D=D, C=C, N=N, R=R, E=E, F=F, chips=chips, T=T, tiles=tiles, slots=slots)
        k_i = lax.broadcasted_iota(jnp.int32, (S, slots, tiles, B), 1)
        t_i = lax.broadcasted_iota(jnp.int32, (S, slots, tiles, B), 2)
        ids4 = expert_ids.reshape(S, 1, 1, B)
        lo = jnp.sum((ids4 < k_i - t_i).astype(jnp.int32), axis=3)
        hi = jnp.sum((ids4 <= k_i - t_i).astype(jnp.int32), axis=3)
        t3 = lax.broadcasted_iota(jnp.int32, (S, slots, tiles), 2)
        tile_of = jnp.max(jnp.where((hi > lo) & (lo < T * (t3 + 1)) & (hi > T * t3), t3, 0), axis=2)
        row = lambda a: a.reshape(1, a.shape[0])
        vm = pl.BlockSpec(memory_space=pltpu.VMEM)
        anym = pl.BlockSpec(memory_space=pl.ANY)
        half, quarter, eighth = B // 2, B // 8, B // 16
        ring = lambda: [
            pltpu.VMEM((S, B, D), BF), pltpu.VMEM((S, half, D), BF),
            pltpu.VMEM((S, 2, eighth, D), BF), pltpu.VMEM((S, 2, eighth, D), BF), pltpu.VMEM((S, 2, eighth, D), BF),
            pltpu.VMEM((S, 2, eighth, D), BF), pltpu.VMEM((S, 2, eighth, D), BF), pltpu.VMEM((S, 2, eighth, D), BF)]
        n_remote = S * (8 + 2 * 7 + 2 * 8)
        JB = B // C
        scratch = [
            pltpu.VMEM((S, B, D), BF), pltpu.VMEM((3, B, C), BF), pltpu.VMEM((3 + S, JB, C, C), BF), pltpu.VMEM((N, B, C), F32),
            pltpu.VMEM((E, D, F), BF), pltpu.VMEM((E, D, F), BF), pltpu.VMEM((E, F, D), BF),
            pltpu.VMEM((2 * C, D), BF), pltpu.VMEM((N, C, C), F32), pltpu.VMEM((7, C, C), F32), pltpu.VMEM((2 * R, C), F32),
            pltpu.VMEM((B, D), BF), pltpu.VMEM((S, JB, C, C), BF), pltpu.VMEM((S, JB, C, C), BF), pltpu.VMEM((S, B, C), F32),
            pltpu.VMEM((B, C), F32), pltpu.VMEM((S, B, B), BF), pltpu.VMEM((S, B, slots * T), BF), pltpu.VMEM((tiles, T, D), BF),
            pltpu.VMEM((-(-slots // 4), T, F), BF), pltpu.VMEM((slots * T, D), BF),
            pltpu.VMEM((S, JB, 2 * R, C), F32), pltpu.VMEM((S, JB, R, C), F32), pltpu.VMEM((S, JB, R, C), F32),
            pltpu.VMEM((S, 3, R, C), F32), pltpu.VMEM((S, JB, 2 * R, C), F32),
            pltpu.VMEM((JB, C, C), F32), pltpu.VMEM((JB, C, C), F32), pltpu.VMEM((JB, C, C), BF),
            *ring(), *ring(),
            pltpu.VMEM((S, quarter, D), BF), pltpu.VMEM((S, quarter, C), F32),
            pltpu.VMEM((S, B, D), BF), pltpu.VMEM((S, B, D), BF),
            pltpu.SemaphoreType.DMA((2 * S + 2 + 2 * N + 3,)),
            pltpu.SemaphoreType.DMA((n_remote,)), pltpu.SemaphoreType.DMA((n_remote,)),
        ]
        y, conv_o, ssm_o = pl.pallas_call(
            functools.partial(layer_kernel, cfg),
            out_shape=(jax.ShapeDtypeStruct((S, B, D), BF), jax.ShapeDtypeStruct((3, B, C), BF), jax.ShapeDtypeStruct((B, N, C), F32)),
            in_specs=[anym] * 3 + [pl.BlockSpec(memory_space=pltpu.SMEM)] + [vm] * 16 + [anym] * 3,
            out_specs=(anym, anym, anym),
            scratch_shapes=scratch,
            compiler_params=pltpu.CompilerParams(collective_id=0, has_side_effects=True, vmem_limit_bytes=62 * 1024 * 1024),
            name="layer_steps",
        )(x_steps, conv_state.transpose(2, 0, 1), ssm_state.transpose(0, 2, 1), tile_of, expert_ids.transpose(0, 2, 1), row(g_in), row(g_ff),
          row(g_dt), row(g_b), row(g_c), w_in.reshape(2 * D, C), conv_w.T, row(conv_b), w_xp.T, w_dt, row(b_dt), a_log.T, row(d_skip),
          w_out, w_router.T, w_gate, w_up, w_down)
        return y, conv_o.transpose(1, 2, 0), ssm_o.transpose(0, 2, 1)

    return jax.shard_map(layer_steps, mesh=mesh, in_specs=in_specs, out_specs=out_specs, check_vma=False)
```
